32 devices in a mesh: vocab: 16 (over z, y, core), tok: 2 (over x).
Axes of the slice: x: 2, y: 2, z: 4, core: 2. Of those that a mesh axis runs over, the one named last changes fastest.
Arguments:
- hidden: bfloat16 [2048, 4096], P('tok', 'vocab'), may hold values from -64 to 64
- weight: bfloat16 [4096, 16384], P(None, 'vocab'), may hold values from -1 to 1
- proj_in: bfloat16 [4096, 64], replicated, may hold values from -0.09375 to 0.09375
- proj_out: bfloat16 [16384, 64], P('vocab'), may hold values from -6 to 6
- targets: int32 [2048], P('tok'), may hold values from 0 to 16383
- segments: int32 [2, 1024], P('tok'), may hold values from 0 to 15, never falling along the last dimension, each value on 1 to 128 neighbouring positions
- queries: bfloat16 [2048, 4096], P(('vocab', 'tok')), may hold values from -0.059814453 to 0.059814453
Outputs:
- scores: float32 [32, 2048], P(None, ('vocab', 'tok'))
The draws below stay inside these ranges and needn't reach their ends.
Inputs may be any that keep to these rules, and one draw needn't show every extreme that they name: `segments`: each group's row numbers its documents 0 to 15 in order, each with 1 to 128 tokens.
All inputs are finite; a program needn't handle non-finite values.
Results may differ from the reference program's by a relative error of at most 0.0095.
Values may be sent and summed in bfloat16 or wider, within the bound.
A program may use at most 64 MiB of HBM per device.

```python
import math
import jax
import jax.numpy as jnp
import numpy as np
from jax import lax

D = 4096
RANK = 64
TOK_DEV = 1024
VOCAB = 16384
GROUPS = 2
TOKENS = 2048
DOCS_G = 16
MOST = 128
DOCS = 32
QUERIES = 2048


def weight_table(key):
    return jax.random.truncated_normal(jax.random.fold_in(key, 11), -6.0, 6.0, (D, VOCAB), jnp.float32) / jnp.sqrt(jnp.float32(D))


def draw_weight(key, part):
    return weight_table(key).astype(jnp.bfloat16)


def draw_hidden(key, part):
    states = 3.0 * jax.random.truncated_normal(jax.random.fold_in(key, 12), -4.0, 4.0, (TOKENS, D), jnp.float32)
    return states.astype(jnp.bfloat16)


def with_ends(drawn, rng, least, largest):
    dims = drawn.shape
    place = [jax.random.randint(jax.random.fold_in(rng, axis), (), 0, dims[axis]) for axis in range(len(dims))]
    drawn = drawn.at[tuple(place)].set(least)
    longest = dims.index(max(dims))
    place[longest] = (place[longest] + 1) % dims[longest]
    return drawn.at[tuple(place)].set(largest)


def block_levels(own_key, shape, pieces, smallest, high):
    factor_of = 1.0
    for dim, shards_of in pieces:
        draws = jax.random.uniform(jax.random.fold_in(jax.random.fold_in(own_key, 6), dim), (shards_of,), jnp.float32, smallest / len(pieces), high / len(pieces))
        factor_of = factor_of * jnp.repeat(jnp.exp(draws), shape[dim] // shards_of).reshape((-1,) + (1,) * (len(shape) - 1 - dim))
    return factor_of


def profile(count, total, most, skew):
    loads = [(1 << 20) // math.isqrt(grade ** skew) + 1 for grade in range(2, count + 1)]
    rest, holding = total - most - (count - 1), [1] * (count - 1)
    while rest > 0:
        candidates = [i for i in range(count - 1) if holding[i] < most]
        pool, remaining = sum([loads[i] for i in candidates]), rest
        for i in candidates:
            addition = min(most - holding[i], max(1, remaining * loads[i] // pool), rest)
            holding[i] = holding[i] + addition
            rest = rest - addition
    return np.array([most] + holding)


def ragged(key, number_of, total, reach, slope):
    if number_of == 2:
        one = jax.random.randint(key, (), max(1, total - reach), min(reach, total - 1) + 1)
        return jnp.stack([one, total - one])
    lengths = jnp.asarray(profile(number_of, total, reach, slope), jnp.int32)
    couples = (number_of - 1) // 2
    giver, sink = lengths[1:1 + 2 * couples:2], lengths[2:2 + 2 * couples:2]
    slack = jnp.minimum(giver - 1, reach - sink)
    passed = jax.random.randint(jax.random.fold_in(key, 1), (couples,), 0, 1 << 20) % (slack + 1)
    lengths = lengths.at[1:1 + 2 * couples:2].set(giver - passed).at[2:2 + 2 * couples:2].set(sink + passed)
    return lengths[jax.random.permutation(jax.random.fold_in(key, 2), number_of)]


def bell_draw(own_key, dims, scale, limit, pieces=(), kind=jnp.bfloat16):
    level = block_levels(own_key, dims, pieces, -0.22, 0.18) if pieces else 1.0
    array = jax.random.normal(own_key, dims, jnp.float32) * scale * level
    return jnp.minimum(jnp.maximum(array, -limit), limit).astype(kind)


def setup_inputs(seed: int = 0) -> dict:
    splits = jax.random.split(jax.random.key(seed), 8)
    return {
        "hidden": draw_hidden(jax.random.fold_in(splits[7], 71), 0),
        "weight": draw_weight(jax.random.fold_in(splits[7], 71), 0),
        "proj_in": bell_draw(splits[2], (D, RANK), D ** -0.5, 0.09375),
        "proj_out": bell_draw(splits[3], (VOCAB, RANK), 1.0, 6.0, ((0, 16),)),
        "targets": with_ends(jax.random.randint(splits[4], (TOKENS,), 0, VOCAB), jax.random.fold_in(splits[4], 1), 0, VOCAB - 1).astype(jnp.int32),
        "segments": jax.vmap(lambda own: jnp.searchsorted(jnp.cumsum(ragged(own, DOCS_G, TOK_DEV, MOST, 2)), jnp.arange(TOK_DEV), side="right"))(jax.random.split(splits[5], GROUPS)).reshape((GROUPS, TOK_DEV)).astype(jnp.int32),
        "queries": bell_draw(splits[6], (QUERIES, RANK * RANK), 0.01, 0.059814453, ((0, 32),)),
    }


def outer_sums(member, left_side, right_side):
    spread = (member[:, :, None] * left_side[:, None, :]).reshape(left_side.shape[0], -1)
    result = lax.dot_general(spread, right_side, (((0,), (0,)), ((), ())), precision=lax.Precision.HIGHEST, preferred_element_type=jnp.float32)
    return result.reshape(member.shape[1], -1)


def reference(hidden, weight, proj_in, proj_out, targets, segments, queries):
    def one_group(inputs):
        states, wanted, labels = inputs
        logits = jnp.dot(states, weight, preferred_element_type=jnp.float32)
        top = jnp.max(logits, axis=1, keepdims=True)
        expo = jnp.exp(logits - top)
        total = jnp.sum(expo, axis=1, keepdims=True)
        column = jnp.arange(VOCAB, dtype=jnp.int32)
        onehot = (wanted[:, None] == column[None, :]).astype(jnp.float32)
        resid = (expo / total - onehot).astype(jnp.bfloat16)
        right_side = jnp.dot(resid, proj_out, preferred_element_type=jnp.float32)
        left_side = jnp.dot(states, proj_in, preferred_element_type=jnp.float32)
        member = (labels[:, None] == jnp.arange(DOCS_G, dtype=jnp.int32)[None, :]).astype(jnp.float32)
        return outer_sums(member, left_side, right_side).astype(jnp.bfloat16)

    grads = lax.map(one_group, (hidden.reshape(GROUPS, TOK_DEV, D), targets.reshape(GROUPS, TOK_DEV), segments))
    doc_grad = grads.reshape(DOCS, RANK * RANK)
    return lax.dot_general(doc_grad, queries, (((1,), (1,)), ((), ())), preferred_element_type=jnp.float32)
```

```python
import functools

import jax
import jax.numpy as jnp
from jax import lax
from jax.experimental import pallas as pl
from jax.experimental.pallas import tpu as pltpu
from jax.sharding import PartitionSpec as P

DOC_V = 1
MESH = pl.DeviceIdType.MESH
LANES = 128
BLOCK = 16
AHEAD = 2
ACROSS = (((1,), (1,)), ((), ()))


def chip_of(place, chips):
    back = place // (chips // 2)
    return (1 - back) * 2 * place + back * (2 * (chips - 1 - place) + 1)


def place_of(chip, chips):
    odd, half = chip % 2, chip // 2
    return odd * (chips - 1 - half) + (1 - odd) * half


def wavefront(chunks, steps):
    order = [(c, 0) for c in range(min(AHEAD, chunks))]
    for k in range(chunks + steps):
        if AHEAD + k < chunks:
            order.append((AHEAD + k, 0))
        for s in range(1, steps):
            if 0 <= k + 1 - s < chunks:
                order.append((k + 1 - s, s))
    return order


def kernel(
    devices, groups, chunks,
    h_hbm, w_hbm, pin_hbm, po_hbm, tgt_hbm, seg_hbm, q_hbm,
    out_ref,
    h_ref, held, w_ref, pin_ref, po_ref, tgt_ref, seg_ref, qs, logits, left, shift, pb_ref, pa_ref,
    hot, turned, spread, msg, stat, got_mate, got_pack, comb, small, got_msg, got_stat,
    rights, grads, flat, scores,
    load_sem, ring_send, ring_recv, mate_send, mate_recv, own_send, own_recv,
    pair_send, pair_recv, msg_send, msg_recv, stat_send, stat_recv, right_send, right_recv,
    q_send, q_recv, group_send, group_recv,
):
    chips, steps = devices // 2, devices // 4
    tokens, depth = h_ref.shape
    vocab = w_ref.shape[1]
    rank = po_ref.shape[0]
    size = tokens // chunks
    half = size // 2
    block = half // chips
    docs = out_ref.shape[0] // groups
    number = out_ref.shape[1]
    group = lax.axis_index("tok")
    me = lax.axis_index("vocab")
    core = me % 2
    chip = me // 2
    place = place_of(chip, chips)
    mate = me + 1 - 2 * core
    nexts = [
        2 * chip_of((place + 1) % chips, chips) + core,
        2 * chip_of((place + chips - 1) % chips, chips) + core,
    ]

    loads = []
    for n, (src, dst) in enumerate([
        (h_hbm, h_ref), (tgt_hbm, tgt_ref), (po_hbm, po_ref), (w_hbm, w_ref), (pin_hbm, pin_ref),
        (seg_hbm, seg_ref), (q_hbm, qs.at[0]),
    ]):
        loads.append(pltpu.make_async_copy(src, dst, load_sem.at[n]))
    h_load, tgt_load, po_load, w_load, pin_load, seg_load, q_load = loads
    h_load.start()

    barrier = pltpu.get_barrier_semaphore()
    for device in nexts + [mate]:
        pl.semaphore_signal(
            barrier, inc=1, device_id={"vocab": device}, device_id_type=MESH
        )
    for k in range(1, groups):
        pl.semaphore_signal(
            barrier, inc=1, device_id={"tok": (group + k) % groups}, device_id_type=MESH
        )
    for each in loads[1:]:
        each.start()
    h_load.wait()
    pl.semaphore_wait(barrier, groups + 2)

    sent = []

    def remote(src, dst, send_sem, recv_sem, device, other=None):
        target = {"vocab": device} if other is None else {"tok": other}
        return pltpu.make_async_remote_copy(
            src_ref=src, dst_ref=dst, send_sem=send_sem, recv_sem=recv_sem,
            device_id=target, device_id_type=MESH,
        )

    def start(*args):
        copy = remote(*args)
        copy.start()
        sent.append(copy)

    def source_of(way, step):
        hops = (chips - step) if way == 0 else step
        return 2 * chip_of((place + hops) % chips, chips) + core

    def rows_of(c, s, way):
        if s == steps - 1:
            return pl.ds(c * size + way * half, half)
        return pl.ds(c * size, size)

    def piece(slot, c, s, way):
        return held.at[slot, rows_of(c, s, way), :]

    def begin(c):
        for way in range(2):
            start(
                h_ref.at[rows_of(c, 0, way), :], piece(me, c, 0, way),
                ring_send.at[way, 0, c], ring_recv.at[way, 0, c], nexts[way],
            )

    def arrive(c, s):
        for way in range(2):
            slot = source_of(way, s + 1)
            here = piece(slot, c, s, way)
            remote(
                here, here, ring_send.at[way, s, c], ring_recv.at[way, s, c], nexts[way]
            ).wait_recv()
            if s + 1 < steps:
                on = piece(slot, c, s + 1, way)
                start(
                    on, on, ring_send.at[way, s + 1, c], ring_recv.at[way, s + 1, c], nexts[way]
                )
            start(here, here, mate_send.at[way, s, c], mate_recv.at[way, s, c], mate)

    def own(c):
        rows = pl.ds(c * size, size)
        return h_ref.at[rows, :], held.at[me, rows, :], own_send.at[c], own_recv.at[c], mate

    wide = 512 if vocab % 512 == 0 else vocab

    def consume(c, loaders, first=False):
        rows = pl.ds(c * size, size)

        def body(n, carry):
            cols = pl.ds(pl.multiple_of(n * wide, wide), wide)
            value = 0.0 if first else logits[rows, cols]
            for load, slot in loaders:
                deep = pl.ds(pl.multiple_of(slot * depth, depth), depth)
                value += jnp.dot(load(rows), w_ref[deep, cols], preferred_element_type=jnp.float32)
            logits[rows, cols] = value
            return carry

        lax.fori_loop(0, vocab // wide, body, 0)
        side = 0.0 if first else left[rows, 0:rank]
        for load, slot in loaders:
            deep = pl.ds(pl.multiple_of(slot * depth, depth), depth)
            side += lax.dot_general(
                load(rows), pin_ref[:, deep], ACROSS, preferred_element_type=jnp.float32
            )
        left[rows, 0:rank] = side

    def consume_own(c):
        remote(*own(c)).wait_recv()
        consume(
            c,
            [(lambda rows: h_ref[rows, :], me), (lambda rows: held[mate, rows, :], mate)],
            first=True,
        )

    def consume_step(c, s):
        flip = 1 - 2 * core
        for way in range(2):
            there = piece(source_of(way, s + 1) + flip, c, s, way)
            remote(
                there, there, mate_send.at[way, s, c], mate_recv.at[way, s, c], mate
            ).wait_recv()
        loaders = []
        for way in range(2 if s < steps - 1 else 1):
            slot = source_of(way, s + 1)
            for each in (slot, slot + flip):
                loaders.append((lambda rows, each=each: held[each, rows, :], each))
        consume(c, loaders)

    lane = lax.broadcasted_iota(jnp.int32, (LANES, LANES), 1)
    inside = lane < rank
    base = lax.broadcasted_iota(jnp.int32, (LANES, vocab), 1) // LANES * LANES

    def spread_lanes(value):
        return jnp.concatenate([value] * (vocab // LANES), axis=1)

    def prepare():
        pa_ref[...] = jnp.zeros_like(pa_ref)
        pb_ref[...] = jnp.zeros_like(pb_ref)
        left[...] = jnp.zeros_like(left)
        grads[...] = jnp.zeros_like(grads)
        tgt_load.wait()
        po_load.wait()
        pa_ref[0:rank, :] = po_ref[...]
        pb_ref[rank : 2 * rank, :] = po_ref[...]

        def mark(i, carry):
            rows = pl.ds(pl.multiple_of(i * LANES, LANES), LANES)
            wanted = jnp.broadcast_to(tgt_ref[:, rows].astype(jnp.float32), (LANES, LANES))
            wanted = jnp.transpose(wanted).astype(jnp.int32) - me * vocab - lane
            shift[rows, :] = wanted
            onehot = jnp.where(spread_lanes(wanted) == base, 1.0, 0.0).astype(jnp.bfloat16)
            hot[rows, :] = lax.dot_general(
                onehot, pb_ref[...], ACROSS, preferred_element_type=jnp.float32
            )
            return carry

        lax.fori_loop(0, tokens // LANES, mark, 0)

    tiles = half // LANES

    def pair_copies(c, part):
        mine = pl.ds(pl.multiple_of(part * half, LANES), half)
        return [
            (msg.at[c, mine, :], got_mate.at[c], pair_send.at[0, c], pair_recv.at[0, c], mate),
            (stat.at[c, mine, :], got_pack.at[c], pair_send.at[1, c], pair_recv.at[1, c], mate),
        ]

    def pack(values):
        packed = jnp.zeros((LANES, LANES), jnp.float32)
        for at, each in enumerate(values):
            packed = jnp.where(lane == at, each, packed)
        return packed

    def soften(c, part):
        def tile(i, carry):
            spot = pl.ds(pl.multiple_of(part * half + i * LANES, LANES), LANES)
            rows = pl.ds(pl.multiple_of(c * size + part * half + i * LANES, LANES), LANES)
            value = logits[rows, :]
            top = jnp.max(value, axis=1, keepdims=True)
            expo = jnp.exp(value - top)
            rest = jnp.where(spread_lanes(shift[rows, :]) == base, 0.0, expo)
            total = jnp.sum(expo, axis=1, keepdims=True)
            others = jnp.sum(rest, axis=1, keepdims=True)
            both = hot[rows, :] + lax.dot_general(
                rest.astype(jnp.bfloat16), pa_ref[...], ACROSS,
                preferred_element_type=jnp.float32,
            )
            msg[c, spot, :] = both.astype(jnp.bfloat16)
            stat[c, spot, :] = pack([top, total, others])
            return carry

        lax.fori_loop(0, tiles, tile, 0)

    def soften_mate(c):
        soften(c, 1 - core)
        for copy in pair_copies(c, 1 - core):
            start(*copy)

    def soften_own(c):
        soften(c, core)

    def rs_copies(c, there):
        peer = 2 * there + core
        away = (there + chips - chip) % chips
        rows = pl.ds(pl.multiple_of(there * block, block), block)
        return [
            (comb.at[c, rows, :], got_msg.at[c, chip], msg_send.at[c, away], msg_recv.at[c, away],
             peer),
            (small.at[c, there], got_stat.at[c, chip], stat_send.at[c, away],
             stat_recv.at[c, away], peer),
        ]

    def join(c):
        for copy in pair_copies(c, core):
            remote(*copy).wait_recv()
        row = lax.broadcasted_iota(jnp.int32, (8, LANES), 0)
        spot = lax.broadcasted_iota(jnp.int32, (8, LANES), 1) // block
        keep = jnp.logical_and(row == spot, row < 3)
        per = LANES // block
        for i in range(tiles):
            at = pl.ds(i * LANES, LANES)
            rows = pl.ds(pl.multiple_of(core * half + i * LANES, LANES), LANES)
            a, b = stat[c, rows, :], got_pack[c, at, :]
            top = jnp.maximum(a[:, 0:1], b[:, 0:1])
            sa, sb = jnp.exp(a[:, 0:1] - top), jnp.exp(b[:, 0:1] - top)
            total = sa * a[:, 1:2] + sb * b[:, 1:2]
            others = sa * a[:, 2:3] + sb * b[:, 2:3]
            both = (
                jnp.where(inside, sa, 1.0) * msg[c, rows, :].astype(jnp.float32)
                + jnp.where(inside, sb, 1.0) * got_mate[c, at, :].astype(jnp.float32)
            )
            comb[c, at, :] = both.astype(jnp.bfloat16)
            line = jnp.transpose(pack([top, total, others]))[0:8, :]
            line = pltpu.roll(line, 0, 1, stride=block, stride_axis=0)
            for k in range(per):
                turn = pltpu.roll(line, (LANES - k * block) % LANES, 1)
                small[c, i * per + k] = jnp.sum(
                    jnp.where(keep, turn, 0.0), axis=0, keepdims=True
                )
        for k in range(1, chips):
            for copy in rs_copies(c, (chip + k) % chips):
                remote(*copy).start()
        got_msg[c, chip] = comb[c, pl.ds(pl.multiple_of(chip * block, block), block), :]
        got_stat[c, chip] = small[c, chip]

    place_in = core * chips + chip

    def gather_copy(c, k):
        peer = (me + k) % devices
        spot = rights.at[c, place_in]
        return spot, spot, right_send.at[c, k], right_recv.at[c, k], peer

    def reduce(c):
        for k in range(1, chips):
            there = (chip + chips - k) % chips
            for dst, send, recv in (
                (got_msg.at[c, there], msg_send.at[c, k], msg_recv.at[c, k]),
                (got_stat.at[c, there], stat_send.at[c, k], stat_recv.at[c, k]),
            ):
                remote(dst, dst, send, recv, 2 * there + core).wait_recv()
        lines = jnp.concatenate([got_stat[c, d] for d in range(chips)], axis=0)
        top = jnp.max(lines, axis=0, keepdims=True)
        scale = jnp.exp(lines - top)
        total = jnp.sum(scale * pltpu.roll(lines, LANES - block, 1), axis=0, keepdims=True)
        others = jnp.sum(scale * pltpu.roll(lines, LANES - 2 * block, 1), axis=0, keepdims=True)
        table = jnp.concatenate(
            [
                scale / total,
                jnp.broadcast_to(others / total, (8, LANES)),
                jnp.zeros((LANES - chips - 8, LANES), jnp.float32),
            ],
            axis=0,
        )
        table = jnp.transpose(table)[0:block, :]
        summed = jnp.zeros((block, LANES), jnp.float32)
        plain = jnp.zeros((block, LANES), jnp.float32)
        for d in range(chips):
            value = got_msg[c, d].astype(jnp.float32)
            summed += value * table[:, d : d + 1]
            plain += value
        right = summed - table[:, chips : chips + 1] * pltpu.roll(plain, rank, 1)
        low, high = right[0 : block // 2, :], right[block // 2 : block, :]
        packed = jnp.where(inside[0 : block // 2, :], low, pltpu.roll(high, rank, 1))
        rights[c, place_in] = packed.astype(jnp.bfloat16)
        for k in range(1, devices):
            start(*gather_copy(c, k))

    def mark_docs(c):
        cols = pl.ds(c * size, size)
        turned[...] = jnp.transpose(left[cols, :])
        member = seg_ref[:, cols] == lax.broadcasted_iota(jnp.int32, (docs, size), 0)

        def body(p, carry):
            rows = pl.ds(pl.multiple_of(p * docs, docs), docs)
            for side in range(2):
                line = turned[pl.ds(2 * p + side, 1), :]
                spread[c, rows, side * size : (side + 1) * size] = jnp.where(
                    member, line, 0.0
                ).astype(jnp.bfloat16)
            return carry

        lax.fori_loop(0, rank // 2, body, 0)

    def add_docs(c):
        for k in range(1, devices):
            peer = (me + devices - k) % devices
            spot = rights.at[c, peer % 2 * chips + peer // 2]
            remote(spot, spot, right_send.at[c, k], right_recv.at[c, k], peer).wait_recv()
        part = block // 2
        packed = rights[c].astype(jnp.float32).reshape(devices * part, LANES)
        moved = pltpu.roll(packed, rank, 1)
        both = jnp.concatenate(
            [packed.reshape(devices, 1, part, LANES), moved.reshape(devices, 1, part, LANES)],
            axis=1,
        ).reshape(size, LANES)
        within = lax.broadcasted_iota(jnp.int32, (size, LANES), 1) < rank
        sides = jnp.concatenate(
            [jnp.where(within, both, 0.0), jnp.where(within, 0.0, pltpu.roll(both, rank, 1))],
            axis=0,
        ).astype(jnp.bfloat16)
        grads[...] += jnp.dot(spread[c], sides, preferred_element_type=jnp.float32)

    order = wavefront(chunks, steps)
    ahead = min(AHEAD, chunks)
    for c in range(ahead):
        begin(c)
    for c in range(chunks):
        start(*own(c))
    for k in range(1, groups):
        start(
            q_hbm, qs.at[groups - k], q_send.at[k], q_recv.at[k], None, (group + k) % groups
        )
    prepare()
    w_load.wait()
    pin_load.wait()
    seg_load.wait()
    for c in range(ahead):
        consume_own(c)

    extra = [functools.partial(consume_own, c) for c in range(ahead, chunks)]
    waiting, ends = [], []

    def finish(c):
        arrive(c, steps - 1)
        waiting.append((c, steps - 1))

    def work():
        while waiting:
            c, s = waiting.pop(0)
            consume_step(c, s)
            if s == steps - 1 and c < chunks - 1:
                extra.extend([
                    functools.partial(soften_mate, c), functools.partial(soften_own, c),
                    functools.partial(join, c), functools.partial(mark_docs, c),
                ])
        for _ in range(2):
            if extra:
                extra.pop(0)()

    for n, (c, s) in enumerate(order[ahead:]):
        if s == 0:
            begin(c)
            continue
        now = list(waiting)
        arrive(c, s - 1)
        work()
        waiting.append((c, s - 1))
        if s == steps - 1:
            ends.append((n + 2, c))
        while ends and ends[0][0] <= n and len(ends) > 1:
            finish(ends.pop(0)[1])
    last = chunks - 1
    while ends:
        finish(ends.pop(0)[1])
        if ends:
            work()
    while extra:
        extra.pop(0)()
    for c in range(max(last - 1, 0)):
        reduce(c)
    work()
    while extra:
        extra.pop(0)()
    soften_mate(last)
    soften_own(last)
    join(last)
    if last > 0:
        reduce(last - 1)
    mark_docs(last)
    for c in range(last):
        add_docs(c)
    reduce(last)
    q_load.wait()
    for k in range(1, groups):
        remote(
            qs.at[k], qs.at[k], q_send.at[groups - k], q_recv.at[groups - k], None,
            (group + k) % groups,
        ).wait_recv()
    add_docs(last)

    for p in range(rank // 2):
        flat[:, p * LANES : (p + 1) * LANES] = grads[p * docs : (p + 1) * docs, :].astype(
            jnp.bfloat16
        )
    mine = pl.ds(pl.multiple_of(group * docs, docs), docs)
    for k in [*range(1, groups), 0]:
        value = lax.dot_general(flat[...], qs[k], ACROSS, preferred_element_type=jnp.float32)
        if k == 0:
            out_ref[mine, :] = value
        else:
            scores[k] = value
            start(
                scores.at[k], out_ref.at[mine, :], group_send.at[k], group_recv.at[k], None,
                (group + k) % groups,
            )
    for k in range(1, groups):
        other = (group + groups - k) % groups
        theirs = out_ref.at[pl.ds(pl.multiple_of(other * docs, docs), docs), :]
        remote(
            theirs, theirs, group_send.at[k], group_recv.at[k], None, other
        ).wait_recv()
    for c in range(chunks):
        for k in range(1, chips):
            for copy in rs_copies(c, (chip + k) % chips):
                remote(*copy).wait_send()
    for copy in sent:
        copy.wait_send()


def attribution(devices, groups, hidden, weight, proj_in, proj_out, targets, segments, queries):
    tokens, depth = hidden.shape
    width, vocab = weight.shape
    rank = proj_in.shape[1]
    number = queries.shape[0]
    docs = DOC_V * devices
    chips, steps = devices // 2, devices // 4
    chunks = max(1, min(4, tokens // (2 * chips * BLOCK)))
    size = tokens // chunks
    half = size // 2
    block = half // chips
    hbm = pl.BlockSpec(memory_space=pl.ANY)
    dma = pltpu.SemaphoreType.DMA
    ring = dma((2, steps, chunks))
    once = dma((chunks,))
    pair = dma((2, chunks))
    peers = dma((chunks, chips))
    everyone = dma((chunks, devices))
    across = dma((groups,))
    f32, bf16 = jnp.float32, jnp.bfloat16
    return pl.pallas_call(
        functools.partial(kernel, devices, groups, chunks),
        out_shape=jax.ShapeDtypeStruct((groups * docs, number), f32),
        in_specs=[hbm] * 7,
        out_specs=pl.BlockSpec(memory_space=pltpu.VMEM),
        scratch_shapes=[
            pltpu.VMEM((tokens, depth), bf16),
            pltpu.VMEM((devices, tokens, depth), bf16),
            pltpu.VMEM((width, vocab), bf16),
            pltpu.VMEM((rank, width), bf16),
            pltpu.VMEM((rank, vocab), bf16),
            pltpu.VMEM((1, tokens), jnp.int32),
            pltpu.VMEM((1, tokens), jnp.int32),
            pltpu.VMEM((groups, number, rank * rank), bf16),
            pltpu.VMEM((tokens, vocab), f32),
            pltpu.VMEM((tokens, LANES), f32),
            pltpu.VMEM((tokens, LANES), jnp.int32),
            pltpu.VMEM((LANES, vocab), bf16),
            pltpu.VMEM((LANES, vocab), bf16),
            pltpu.VMEM((tokens, LANES), f32),
            pltpu.VMEM((LANES, size), f32),
            pltpu.VMEM((chunks, docs * rank // 2, 2 * size), bf16),
            pltpu.VMEM((chunks, size, LANES), bf16),
            pltpu.VMEM((chunks, size, LANES), f32),
            pltpu.VMEM((chunks, half, LANES), bf16),
            pltpu.VMEM((chunks, half, LANES), f32),
            pltpu.VMEM((chunks, half, LANES), bf16),
            pltpu.VMEM((chunks, chips, 1, LANES), f32),
            pltpu.VMEM((chunks, chips, block, LANES), bf16),
            pltpu.VMEM((chunks, chips, 1, LANES), f32),
            pltpu.VMEM((chunks, devices, block // 2, LANES), bf16),
            pltpu.VMEM((docs * rank // 2, LANES), f32),
            pltpu.VMEM((docs, rank * rank), bf16),
            pltpu.VMEM((groups, docs, number), f32),
            dma((7,)), ring, ring, ring, ring, once, once, pair, pair,
            peers, peers, peers, peers, everyone, everyone, across, across, across, across,
        ],
        compiler_params=pltpu.CompilerParams(
            collective_id=0, has_side_effects=True, vmem_limit_bytes=60 * 1024 * 1024
        ),
    )(
        hidden, weight, proj_in.T, proj_out.T, targets[None, :], segments, queries,
    )


def solution(mesh):
    devices, groups = mesh.shape["vocab"], mesh.shape["tok"]
    return jax.shard_map(
        functools.partial(attribution, devices, groups),
        mesh=mesh,
        in_specs=(
            P("tok", "vocab"),
            P(None, "vocab"),
            P(),
            P("vocab", None),
            P("tok"),
            P("tok", None),
            P(("vocab", "tok"), None),
        ),
        out_specs=P(None, ("vocab", "tok")),
        check_vma=False,
    )
```

```python
import functools

import jax
import jax.numpy as jnp
from jax import lax
from jax.experimental import pallas as pl
from jax.experimental.pallas import tpu as pltpu
from jax.sharding import PartitionSpec as P

DOC_V = 1
MESH = pl.DeviceIdType.MESH
LANES = 128
BLOCK = 16
AHEAD = 2
HOLD = 5
ACROSS = (((1,), (1,)), ((), ()))


def chip_of(place, chips):
    back = place // (chips // 2)
    return (1 - back) * 2 * place + back * (2 * (chips - 1 - place) + 1)


def place_of(chip, chips):
    odd, half = chip % 2, chip // 2
    return odd * (chips - 1 - half) + (1 - odd) * half


def wavefront(chunks, steps):
    order = [(c, 0) for c in range(min(AHEAD, chunks))]
    for k in range(chunks + steps):
        if AHEAD + k < chunks:
            order.append((AHEAD + k, 0))
        for s in range(1, steps):
            if 0 <= k + 1 - s < chunks:
                order.append((k + 1 - s, s))
    return order


def kernel(
    devices, groups, chunks,
    h_hbm, w_hbm, pin_hbm, po_hbm, tgt_hbm, seg_hbm, q_hbm,
    out_ref,
    h_ref, held, w_ref, pin_ref, tgt_ref, seg_ref, qs, logits, left, shift, pb_ref, pa_ref,
    hot, turned, spread, msg, small, got_msg, got_stat, rights,
    hot_late, got_hot, hot_sum, msg_late, got_late, line_late, got_line, rights_late,
    grads, flat, scores,
    load_sem, ring_send, ring_recv, side_send, side_recv, own_send, own_recv,
    mate_send, mate_recv, left_send, left_recv,
    msg_send, msg_recv, stat_send, stat_recv, right_send, right_recv,
    late_send, late_recv, swap_send, swap_recv, q_send, q_recv, group_send, group_recv,
):
    chips, steps = devices // 2, devices // 4
    tokens, depth = h_ref.shape
    vocab = w_ref.shape[2]
    rank = po_hbm.shape[0]
    size = tokens // chunks
    half = size // 2
    block = half // chips
    docs = out_ref.shape[0] // groups
    number = out_ref.shape[1]
    last = chunks - 1
    group = lax.axis_index("tok")
    me = lax.axis_index("vocab")
    core = me % 2
    chip = me // 2
    place = place_of(chip, chips)
    mate = me + 1 - 2 * core
    nexts = [
        2 * chip_of((place + 1) % chips, chips) + core,
        2 * chip_of((place + chips - 1) % chips, chips) + core,
    ]

    my_cols = pl.ds(pl.multiple_of(core * vocab, vocab), vocab)
    pa_mine, pb_mine = pa_ref.at[0:rank, my_cols], pb_ref.at[rank : 2 * rank, my_cols]
    loads = []
    for n, (src, dst) in enumerate([
        (h_hbm, h_ref), (tgt_hbm, tgt_ref), (po_hbm, pa_mine), (po_hbm, pb_mine),
        (w_hbm, w_ref.at[core]), (pin_hbm, pin_ref), (seg_hbm, seg_ref), (q_hbm, qs.at[pl.ds(0, number), :]),
    ]):
        loads.append(pltpu.make_async_copy(src, dst, load_sem.at[n]))
    h_load, tgt_load, pa_load, pb_load, w_load, pin_load, seg_load, q_load = loads
    h_load.start()

    barrier = pltpu.get_barrier_semaphore()
    for device in nexts + [mate]:
        pl.semaphore_signal(
            barrier, inc=1, device_id={"vocab": device}, device_id_type=MESH
        )
    for k in range(1, groups):
        pl.semaphore_signal(
            barrier, inc=1, device_id={"tok": (group + k) % groups}, device_id_type=MESH
        )
    for each in loads[1:]:
        each.start()
    h_load.wait()
    pl.semaphore_wait(barrier, groups + 2)

    sent = []

    def remote(src, dst, send_sem, recv_sem, device, other=None):
        target = {"vocab": device} if other is None else {"tok": other}
        return pltpu.make_async_remote_copy(
            src_ref=src, dst_ref=dst, send_sem=send_sem, recv_sem=recv_sem,
            device_id=target, device_id_type=MESH,
        )

    def start(*args):
        copy = remote(*args)
        copy.start()
        sent.append(copy)

    def source_of(way, step):
        hops = (chips - step) if way == 0 else step
        return chip_of((place + hops) % chips, chips)

    def tokens_of(c, who):
        return pl.ds(pl.multiple_of(c * size + who * half, LANES), half)

    def piece(slot, c, s, way):
        if s == steps - 1:
            return held.at[slot, pl.ds(c * half + way * (half // 2), half // 2), :]
        return held.at[slot, pl.ds(c * half, half), :]

    def cols_of(who):
        return pl.ds(pl.multiple_of(who * depth, depth), depth)

    def own_part(c, way):
        return (
            h_ref.at[tokens_of(c, core), :],
            held.at[chip, pl.ds(c * half, half), cols_of(core)],
            side_send.at[way, c], side_recv.at[way, c], nexts[way],
        )

    def mate_part(c, way):
        part = held.at[chip, pl.ds(c * half, half), cols_of(1 - core)]
        return part, part, ring_send.at[way, 0, c], ring_recv.at[way, 0, c], nexts[way]

    def swap(c, who):
        return (
            h_ref.at[tokens_of(c, 1 - who), :],
            held.at[chip, pl.ds(c * half, half), cols_of(who)],
            own_send.at[c], own_recv.at[c], mate,
        )

    def begin(c):
        for way in range(2):
            start(*own_part(c, way))

    def begin_mate(c):
        remote(*swap(c, 1 - core)).wait_recv()
        for way in range(2):
            start(*mate_part(c, way))

    def arrive(c, s):
        for way in range(2):
            slot = source_of(way, s + 1)
            if s == 0:
                for who, send, recv in (
                    (core, side_send, side_recv.at[way, c]),
                    (1 - core, side_send, ring_recv.at[way, 0, c]),
                ):
                    here = held.at[slot, pl.ds(c * half, half), cols_of(who)]
                    remote(here, here, send.at[way, c], recv, nexts[way]).wait_recv()
            else:
                here = piece(slot, c, s, way)
                remote(
                    here, here, ring_send.at[way, s, c], ring_recv.at[way, s, c], nexts[way]
                ).wait_recv()
            if s + 1 < steps:
                on = piece(slot, c, s + 1, way)
                start(
                    on, on, ring_send.at[way, s + 1, c], ring_recv.at[way, s + 1, c], nexts[way]
                )

    wide = vocab
    per_core = vocab // wide

    def consume(c, loaders, first=False):
        rows = pl.ds(c * half, half)

        def body(n, carry):
            who = n // per_core
            cols = pl.ds(pl.multiple_of(n % per_core * wide, wide), wide)
            outs = pl.ds(pl.multiple_of(n * wide, wide), wide)
            value = 0.0 if first else logits[rows, outs]
            for load, deep in loaders:
                value += jnp.dot(
                    load(), w_ref[who, deep, cols], preferred_element_type=jnp.float32
                )
            logits[rows, outs] = value
            return carry

        lax.fori_loop(0, 2 * per_core, body, 0)
        side = 0.0 if first else left[c, core, :, 0:rank]
        for load, deep in loaders:
            side += lax.dot_general(
                load(), pin_ref[:, deep], ACROSS, preferred_element_type=jnp.float32
            )
        left[c, core, :, 0:rank] = side

    def deep_of(device):
        return pl.ds(pl.multiple_of(device * depth, depth), depth)

    def own_loaders(c):
        rows = pl.ds(c * half, half)
        return [
            (lambda: h_ref[tokens_of(c, core), :], deep_of(me)),
            (lambda: held[chip, rows, cols_of(1 - core)], deep_of(mate)),
        ]

    def step_loaders(c, s):
        rows = pl.ds(c * half, half)
        loaders = []
        for way in range(2 if s < steps - 1 else 1):
            slot = source_of(way, s + 1)
            deep = pl.ds(pl.multiple_of(slot * 2 * depth, 2 * depth), 2 * depth)
            loaders.append((lambda slot=slot: held[slot, rows, :], deep))
        return loaders

    lane = lax.broadcasted_iota(jnp.int32, (LANES, LANES), 1)
    inside = lane < rank
    base = lax.broadcasted_iota(jnp.int32, (LANES, 2 * vocab), 1) // LANES * LANES

    def spread_lanes(value):
        return jnp.concatenate([value] * (2 * vocab // LANES), axis=1)

    mates = [
        (pa_mine, pa_mine, mate_send.at[0], mate_recv.at[0], mate),
        (pb_mine, pb_mine, mate_send.at[1], mate_recv.at[1], mate),
        (w_hbm, w_ref.at[core], mate_send.at[2], mate_recv.at[2], mate),
    ]
    other_cols = pl.ds(pl.multiple_of((1 - core) * vocab, vocab), vocab)
    theirs = [
        pa_ref.at[0:rank, other_cols], pb_ref.at[rank : 2 * rank, other_cols],
        w_ref.at[1 - core],
    ]

    def from_mate(n):
        remote(theirs[n], theirs[n], mate_send.at[n], mate_recv.at[n], mate).wait_recv()

    def clear():
        pa_ref[rank : 2 * rank, :] = jnp.zeros((rank, 2 * vocab), jnp.bfloat16)
        pb_ref[0:rank, :] = jnp.zeros((rank, 2 * vocab), jnp.bfloat16)
        for c in range(chunks):
            left[c, core] = jnp.zeros((half, LANES), jnp.float32)
        grads[...] = jnp.zeros_like(grads)

    def prepare(c):
        for i in range(tiles):
            rows = pl.ds(c * half + i * LANES, LANES)
            spot = pl.ds(pl.multiple_of(c * size + core * half + i * LANES, LANES), LANES)
            wanted = jnp.broadcast_to(tgt_ref[:, spot].astype(jnp.float32), (LANES, LANES))
            wanted = jnp.transpose(wanted).astype(jnp.int32) - 2 * chip * vocab - lane
            shift[rows, :] = wanted
            onehot = jnp.where(spread_lanes(wanted) == base, 1.0, 0.0).astype(jnp.bfloat16)
            hot[rows, :] = lax.dot_general(
                onehot, pb_ref[...], ACROSS, preferred_element_type=jnp.float32
            )

    tiles = half // LANES

    def pack(values):
        packed = jnp.zeros((LANES, LANES), jnp.float32)
        for at, each in enumerate(values):
            packed = jnp.where(lane == at, each, packed)
        return packed

    def left_copy(c, who):
        return left.at[c, who], left.at[c, who], left_send.at[c], left_recv.at[c], mate

    def rs_copies(c, there):
        peer = 2 * there + core
        away = (there + chips - chip) % chips
        rows = pl.ds(pl.multiple_of(there * block, block), block)
        return [
            (msg.at[c, rows, :], got_msg.at[c, chip], msg_send.at[c, away], msg_recv.at[c, away],
             peer),
            (small.at[c, there], got_stat.at[c, chip], stat_send.at[c, away],
             stat_recv.at[c, away], peer),
        ]

    def soften(c):
        start(*left_copy(c, core))
        row = lax.broadcasted_iota(jnp.int32, (8, LANES), 0)
        spot = lax.broadcasted_iota(jnp.int32, (8, LANES), 1) // block
        keep = jnp.logical_and(row == spot, row < 3)
        per = LANES // block
        for i in range(tiles):
            rows = pl.ds(c * half + i * LANES, LANES)
            value = logits[rows, :]
            top = jnp.max(value, axis=1, keepdims=True)
            expo = jnp.exp(value - top)
            rest = jnp.where(spread_lanes(shift[rows, :]) == base, 0.0, expo)
            total = jnp.sum(expo, axis=1, keepdims=True)
            others = jnp.sum(rest, axis=1, keepdims=True)
            both = hot[rows, :] + lax.dot_general(
                rest.astype(jnp.bfloat16), pa_ref[...], ACROSS,
                preferred_element_type=jnp.float32,
            )
            msg[c, i * LANES : (i + 1) * LANES, :] = both.astype(jnp.bfloat16)
            line = jnp.transpose(pack([top, total, others]))[0:8, :]
            line = pltpu.roll(line, 0, 1, stride=block, stride_axis=0)
            for k in range(per):
                turn = pltpu.roll(line, (LANES - k * block) % LANES, 1)
                small[c, i * per + k] = jnp.sum(
                    jnp.where(keep, turn, 0.0), axis=0, keepdims=True
                )
        for k in range(1, chips):
            for copy in rs_copies(c, (chip + k) % chips):
                remote(*copy).start()
        got_msg[c, chip] = msg[c, pl.ds(pl.multiple_of(chip * block, block), block), :]
        got_stat[c, chip] = small[c, chip]

    fold = half // 2
    beside = lax.broadcasted_iota(jnp.int32, (fold, LANES), 1) < rank
    late = [(hot_late, got_hot), (msg_late, got_late), (line_late, got_line)]

    def late_copy(n, k):
        src, dst = late[n]
        there = (chip + k) % chips
        return src, dst.at[chip], late_send.at[n, k], late_recv.at[n, k], 2 * there + core

    def late_wait(n):
        for k in range(1, chips):
            there = (chip + chips - k) % chips
            spot = late[n][1].at[there]
            remote(
                spot, spot, late_send.at[n, k], late_recv.at[n, k], 2 * there + core
            ).wait_recv()

    def late_push(n):
        for k in range(1, chips):
            start(*late_copy(n, k))
        late[n][1][chip] = late[n][0][...]

    def push_hot():
        upper = hot[last * half : last * half + fold, :]
        lower = hot[last * half + fold : (last + 1) * half, :]
        hot_late[...] = jnp.where(beside, pltpu.roll(upper, rank, 1), lower).astype(jnp.bfloat16)
        late_push(0)

    def sum_hot():
        late_wait(0)
        value = jnp.zeros((fold, LANES), jnp.float32)
        for d in range(chips):
            value += got_hot[d].astype(jnp.float32)
        hot_sum[...] = value

    def soften_late():
        start(*left_copy(last, core))
        sums = []
        for i in range(tiles):
            rows = pl.ds(last * half + i * LANES, LANES)
            value = logits[rows, :]
            top = jnp.max(value, axis=1, keepdims=True)
            expo = jnp.exp(value - top)
            rest = jnp.where(spread_lanes(shift[rows, :]) == base, 0.0, expo)
            total = jnp.sum(expo, axis=1, keepdims=True)
            others = jnp.sum(rest, axis=1, keepdims=True)
            sums.append(lax.dot_general(
                rest.astype(jnp.bfloat16), pa_ref[...], ACROSS,
                preferred_element_type=jnp.float32,
            ))
            line_late[i] = jnp.transpose(pack([top, total, others]))[0:8, :]
        late_push(2)
        value = jnp.concatenate(sums, axis=0)
        msg_late[...] = jnp.where(
            beside, value[0:fold, :], pltpu.roll(value[fold:half, :], rank, 1)
        ).astype(jnp.bfloat16)
        late_push(1)

    def late_swap(who):
        return rights_late.at[who], rights_late.at[who], swap_send, swap_recv, mate

    def settle_late():
        late_wait(2)
        tables = []
        for i in range(tiles):
            lines = [got_line[d, i] for d in range(chips)]
            top = functools.reduce(jnp.maximum, [each[0:1, :] for each in lines])
            scale = [jnp.exp(each[0:1, :] - top) for each in lines]
            total = sum(scale[d] * lines[d][1:2, :] for d in range(chips))
            others = sum(scale[d] * lines[d][2:3, :] for d in range(chips))
            table = jnp.concatenate(
                [each / total for each in scale]
                + [
                    jnp.broadcast_to(others / total, (8, LANES)),
                    jnp.zeros((LANES - chips - 8, LANES), jnp.float32),
                ],
                axis=0,
            )
            tables.append(jnp.transpose(table))
        table = jnp.concatenate(tables, axis=0)

        def column(d):
            return jnp.where(beside, table[0:fold, d : d + 1], table[fold:half, d : d + 1])

        right = -column(chips) * hot_sum[...]
        factors = [column(d) for d in range(chips)]
        late_wait(1)
        for d in range(chips):
            right += factors[d] * got_late[d].astype(jnp.float32)
        rights_late[core] = right.astype(jnp.bfloat16)
        start(*late_swap(core))

    place_in = core * chips + chip

    def gather_copy(c, k):
        peer = (me + k) % devices
        spot = rights.at[c, place_in]
        return spot, spot, right_send.at[c, k], right_recv.at[c, k], peer

    def reduce(c):
        for k in range(1, chips):
            there = (chip + chips - k) % chips
            for dst, send, recv in (
                (got_msg.at[c, there], msg_send.at[c, k], msg_recv.at[c, k]),
                (got_stat.at[c, there], stat_send.at[c, k], stat_recv.at[c, k]),
            ):
                remote(dst, dst, send, recv, 2 * there + core).wait_recv()
        lines = jnp.concatenate([got_stat[c, d] for d in range(chips)], axis=0)
        top = jnp.max(lines, axis=0, keepdims=True)
        scale = jnp.exp(lines - top)
        total = jnp.sum(scale * pltpu.roll(lines, LANES - block, 1), axis=0, keepdims=True)
        others = jnp.sum(scale * pltpu.roll(lines, LANES - 2 * block, 1), axis=0, keepdims=True)
        table = jnp.concatenate(
            [
                scale / total,
                jnp.broadcast_to(others / total, (8, LANES)),
                jnp.zeros((LANES - chips - 8, LANES), jnp.float32),
            ],
            axis=0,
        )
        table = jnp.transpose(table)[0:block, :]
        summed = jnp.zeros((block, LANES), jnp.float32)
        plain = jnp.zeros((block, LANES), jnp.float32)
        for d in range(chips):
            value = got_msg[c, d].astype(jnp.float32)
            summed += value * table[:, d : d + 1]
            plain += value
        right = summed - table[:, chips : chips + 1] * pltpu.roll(plain, rank, 1)
        low, high = right[0 : block // 2, :], right[block // 2 : block, :]
        packed = jnp.where(inside[0 : block // 2, :], low, pltpu.roll(high, rank, 1))
        rights[c, place_in] = packed.astype(jnp.bfloat16)
        for k in range(1, devices):
            start(*gather_copy(c, k))

    def mark_docs(c):
        cols = pl.ds(c * size, size)
        remote(*left_copy(c, 1 - core)).wait_recv()
        turned[...] = jnp.transpose(left[c].reshape(size, LANES))
        member = seg_ref[:, cols] == lax.broadcasted_iota(jnp.int32, (docs, size), 0)

        def body(p, carry):
            rows = pl.ds(pl.multiple_of(p * docs, docs), docs)
            for side in range(2):
                line = turned[pl.ds(2 * p + side, 1), :]
                spread[c, rows, side * size : (side + 1) * size] = jnp.where(
                    member, line, 0.0
                ).astype(jnp.bfloat16)
            return carry

        lax.fori_loop(0, rank // 2, body, 0)

    def add_docs(c):
        if c == last:
            remote(*late_swap(1 - core)).wait_recv()
            packed, owning = rights_late[...].astype(jnp.float32), 1
        else:
            for k in range(1, devices):
                peer = (me + devices - k) % devices
                spot = rights.at[c, peer % 2 * chips + peer // 2]
                remote(spot, spot, right_send.at[c, k], right_recv.at[c, k], peer).wait_recv()
            packed, owning = rights[c].astype(jnp.float32), chips
        packed = packed.reshape(half, LANES)
        moved = pltpu.roll(packed, rank, 1)
        shape = (2 * owning, 1, fold // owning, LANES)
        both = jnp.concatenate([packed.reshape(shape), moved.reshape(shape)], axis=1)
        both = both.reshape(size, LANES)
        within = lax.broadcasted_iota(jnp.int32, (size, LANES), 1) < rank
        sides = jnp.concatenate(
            [jnp.where(within, both, 0.0), jnp.where(within, 0.0, pltpu.roll(both, rank, 1))],
            axis=0,
        ).astype(jnp.bfloat16)
        grads[...] += jnp.dot(spread[c], sides, preferred_element_type=jnp.float32)

    def query_rows(k):
        return qs.at[pl.ds(k * number, number), :]

    order = wavefront(chunks, steps)
    ahead = min(AHEAD, chunks)
    for c in range(ahead):
        begin(c)
    for c in range(chunks):
        start(*swap(c, core))
    pa_load.wait()
    pb_load.wait()
    for copy in mates:
        start(*copy)
    for k in range(1, groups):
        start(
            q_hbm, query_rows(groups - k), q_send.at[k], q_recv.at[k], None,
            (group + k) % groups,
        )
    for c in range(ahead):
        begin_mate(c)
    clear()
    tgt_load.wait()
    from_mate(0)
    from_mate(1)
    for c in range(chunks):
        prepare(c)

    def weights():
        w_load.wait()
        pin_load.wait()
        seg_load.wait()
        from_mate(2)

    tasks = [weights]
    ready = {c: own_loaders(c) for c in range(chunks)}

    def take(c, s):
        ready[c] += step_loaders(c, s)
        if s % 2 == 0 or s == steps - 1:
            tasks.append(functools.partial(consume, c, ready[c], s == 0))
            ready[c] = []
        if s == steps - 1:
            tasks.append(functools.partial(soften, c))
            if c == 0:
                tasks.append(push_hot)
            tasks.append(functools.partial(mark_docs, c))

    ends = []
    for n, (c, s) in enumerate(order[ahead:]):
        if s == 0:
            begin(c)
            begin_mate(c)
            continue
        arrive(c, s - 1)
        take(c, s - 1)
        if s == steps - 1:
            ends.append((n + 2, c))
        while ends and ends[0][0] <= n and len(ends) > 1:
            c = ends.pop(0)[1]
            arrive(c, steps - 1)
            take(c, steps - 1)
        for _ in range(3):
            if tasks and n >= HOLD:
                tasks.pop(0)()
    while len(ends) > 1:
        c = ends.pop(0)[1]
        arrive(c, steps - 1)
        take(c, steps - 1)
        while tasks:
            tasks.pop(0)()
    while tasks:
        tasks.pop(0)()
    for c in range(last - 1):
        reduce(c)
    sum_hot()
    arrive(last, steps - 1)
    consume(last, step_loaders(last, steps - 1))
    soften_late()
    mark_docs(last)
    if last > 0:
        reduce(last - 1)
    for c in range(last - 1):
        add_docs(c)
    settle_late()
    q_load.wait()
    for k in range(1, groups):
        remote(
            query_rows(k), query_rows(k), q_send.at[groups - k], q_recv.at[groups - k], None,
            (group + k) % groups,
        ).wait_recv()
    for c in range(max(last - 1, 0), chunks):
        add_docs(c)

    for p in range(rank // 2):
        flat[:, p * LANES : (p + 1) * LANES] = grads[p * docs : (p + 1) * docs, :].astype(
            jnp.bfloat16
        )
    mine = pl.ds(pl.multiple_of(group * docs, docs), docs)
    value = lax.dot_general(flat[...], qs[...], ACROSS, preferred_element_type=jnp.float32)
    for k in range(1, groups):
        scores[k] = value[:, k * number : (k + 1) * number]
        start(
            scores.at[k], out_ref.at[mine, :], group_send.at[k], group_recv.at[k], None,
            (group + k) % groups,
        )
    out_ref[mine, :] = value[:, 0:number]
    for k in range(1, groups):
        other = (group + groups - k) % groups
        theirs = out_ref.at[pl.ds(pl.multiple_of(other * docs, docs), docs), :]
        remote(
            theirs, theirs, group_send.at[k], group_recv.at[k], None, other
        ).wait_recv()
    for c in range(last):
        for k in range(1, chips):
            for copy in rs_copies(c, (chip + k) % chips):
                remote(*copy).wait_send()
    for copy in sent:
        copy.wait_send()


def attribution(devices, groups, hidden, weight, proj_in, proj_out, targets, segments, queries):
    tokens, depth = hidden.shape
    width, vocab = weight.shape
    rank = proj_in.shape[1]
    number = queries.shape[0]
    docs = DOC_V * devices
    chips, steps = devices // 2, devices // 4
    chunks = max(1, min(4, tokens // (2 * chips * BLOCK)))
    size = tokens // chunks
    half = size // 2
    block = half // chips
    hbm = pl.BlockSpec(memory_space=pl.ANY)
    dma = pltpu.SemaphoreType.DMA
    ring = dma((2, steps, chunks))
    once = dma((chunks,))
    sides = dma((2, chunks))
    peers = dma((chunks, chips))
    everyone = dma((chunks, devices))
    across = dma((groups,))
    f32, bf16 = jnp.float32, jnp.bfloat16
    return pl.pallas_call(
        functools.partial(kernel, devices, groups, chunks),
        out_shape=jax.ShapeDtypeStruct((groups * docs, number), f32),
        in_specs=[hbm] * 7,
        out_specs=pl.BlockSpec(memory_space=pltpu.VMEM),
        scratch_shapes=[
            pltpu.VMEM((tokens, depth), bf16),
            pltpu.VMEM((chips, tokens // 2, 2 * depth), bf16),
            pltpu.VMEM((2, width, vocab), bf16),
            pltpu.VMEM((rank, width), bf16),
            pltpu.VMEM((1, tokens), jnp.int32),
            pltpu.VMEM((1, tokens), jnp.int32),
            pltpu.VMEM((groups * number, rank * rank), bf16),
            pltpu.VMEM((tokens // 2, 2 * vocab), f32),
            pltpu.VMEM((chunks, 2, half, LANES), f32),
            pltpu.VMEM((tokens // 2, LANES), jnp.int32),
            pltpu.VMEM((LANES, 2 * vocab), bf16),
            pltpu.VMEM((LANES, 2 * vocab), bf16),
            pltpu.VMEM((tokens // 2, LANES), f32),
            pltpu.VMEM((LANES, size), f32),
            pltpu.VMEM((chunks, docs * rank // 2, 2 * size), bf16),
            pltpu.VMEM((chunks, half, LANES), bf16),
            pltpu.VMEM((chunks, chips, 1, LANES), f32),
            pltpu.VMEM((chunks, chips, block, LANES), bf16),
            pltpu.VMEM((chunks, chips, 1, LANES), f32),
            pltpu.VMEM((chunks, devices, block // 2, LANES), bf16),
            pltpu.VMEM((half // 2, LANES), bf16),
            pltpu.VMEM((chips, half // 2, LANES), bf16),
            pltpu.VMEM((half // 2, LANES), f32),
            pltpu.VMEM((half // 2, LANES), bf16),
            pltpu.VMEM((chips, half // 2, LANES), bf16),
            pltpu.VMEM((half // LANES, 8, LANES), f32),
            pltpu.VMEM((chips, half // LANES, 8, LANES), f32),
            pltpu.VMEM((2, half // 2, LANES), bf16),
            pltpu.VMEM((docs * rank // 2, LANES), f32),
            pltpu.VMEM((docs, rank * rank), bf16),
            pltpu.VMEM((groups, docs, number), f32),
            dma((8,)), ring, ring, sides, sides, once, once, dma((3,)), dma((3,)), once, once,
            peers, peers, peers, peers, everyone, everyone, dma((3, chips)), dma((3, chips)),
            dma(()), dma(()), across, across, across, across,
        ],
        compiler_params=pltpu.CompilerParams(
            collective_id=0, has_side_effects=True, vmem_limit_bytes=60 * 1024 * 1024
        ),
    )(
        hidden, weight, proj_in.T, proj_out.T, targets[None, :], segments, queries,
    )


def solution(mesh):
    devices, groups = mesh.shape["vocab"], mesh.shape["tok"]
    return jax.shard_map(
        functools.partial(attribution, devices, groups),
        mesh=mesh,
        in_specs=(
            P("tok", "vocab"),
            P(None, "vocab"),
            P(),
            P("vocab", None),
            P("tok"),
            P("tok", None),
            P(("vocab", "tok"), None),
        ),
        out_specs=P(None, ("vocab", "tok")),
        check_vma=False,
    )
```

```python
import functools

import jax
import jax.numpy as jnp
from jax import lax
from jax.experimental import pallas as pl
from jax.experimental.pallas import tpu as pltpu
from jax.sharding import PartitionSpec as P

DOC_V = 1
MESH = pl.DeviceIdType.MESH
LANES = 128
BLOCK = 16
AHEAD = 2
HOLD = 5
ACROSS = (((1,), (1,)), ((), ()))


def chip_of(place, chips):
    back = place // (chips // 2)
    return (1 - back) * 2 * place + back * (2 * (chips - 1 - place) + 1)


def place_of(chip, chips):
    odd, half = chip % 2, chip // 2
    return odd * (chips - 1 - half) + (1 - odd) * half


def wavefront(chunks, steps):
    order = [(c, 0) for c in range(min(AHEAD, chunks))]
    for k in range(chunks + steps):
        if AHEAD + k < chunks:
            order.append((AHEAD + k, 0))
        for s in range(1, steps):
            if 0 <= k + 1 - s < chunks:
                order.append((k + 1 - s, s))
    return order


def kernel(
    devices, groups, chunks,
    h_hbm, w_hbm, pin_hbm, po_hbm, tgt_hbm, seg_hbm, q_hbm,
    out_ref,
    h_ref, held, w_ref, pin_ref, tgt_ref, seg_ref, qs, logits, left, shift, pb_ref, pa_ref,
    hot, turned, spread, msg, small, got_msg, got_stat, rights,
    hot_late, got_hot, hot_sum, msg_late, got_late, line_late, got_line, rights_late,
    grads, flat, scores,
    load_sem, ring_send, ring_recv, side_send, side_recv, own_send, own_recv,
    mate_send, mate_recv, left_send, left_recv,
    msg_send, msg_recv, stat_send, stat_recv, right_send, right_recv,
    late_send, late_recv, swap_send, swap_recv, q_send, q_recv, group_send, group_recv,
):
    chips, steps = devices // 2, devices // 4
    tokens, depth = h_ref.shape
    vocab = w_ref.shape[2]
    rank = po_hbm.shape[0]
    size = tokens // chunks
    half = size // 2
    block = half // chips
    docs = out_ref.shape[0] // groups
    number = out_ref.shape[1]
    last = chunks - 1
    group = lax.axis_index("tok")
    me = lax.axis_index("vocab")
    core = me % 2
    chip = me // 2
    place = place_of(chip, chips)
    mate = me + 1 - 2 * core
    nexts = [
        2 * chip_of((place + 1) % chips, chips) + core,
        2 * chip_of((place + chips - 1) % chips, chips) + core,
    ]

    my_cols = pl.ds(pl.multiple_of(core * vocab, vocab), vocab)
    pa_mine, pb_mine = pa_ref.at[0:rank, my_cols], pb_ref.at[rank : 2 * rank, my_cols]
    loads = []
    for n, (src, dst) in enumerate([
        (h_hbm, h_ref), (tgt_hbm, tgt_ref), (po_hbm, pa_mine), (po_hbm, pb_mine),
        (w_hbm, w_ref.at[core]), (pin_hbm, pin_ref), (seg_hbm, seg_ref), (q_hbm, qs.at[pl.ds(0, number), :]),
    ]):
        loads.append(pltpu.make_async_copy(src, dst, load_sem.at[n]))
    h_load, tgt_load, pa_load, pb_load, w_load, pin_load, seg_load, q_load = loads
    h_load.start()

    barrier = pltpu.get_barrier_semaphore()
    for device in nexts + [mate]:
        pl.semaphore_signal(
            barrier, inc=1, device_id={"vocab": device}, device_id_type=MESH
        )
    for k in range(1, groups):
        pl.semaphore_signal(
            barrier, inc=1, device_id={"tok": (group + k) % groups}, device_id_type=MESH
        )
    for each in loads[1:]:
        each.start()
    h_load.wait()
    pl.semaphore_wait(barrier, groups + 2)

    sent = []

    def remote(src, dst, send_sem, recv_sem, device, other=None):
        target = {"vocab": device} if other is None else {"tok": other}
        return pltpu.make_async_remote_copy(
            src_ref=src, dst_ref=dst, send_sem=send_sem, recv_sem=recv_sem,
            device_id=target, device_id_type=MESH,
        )

    def start(*args):
        copy = remote(*args)
        copy.start()
        sent.append(copy)

    def source_of(way, step):
        hops = (chips - step) if way == 0 else step
        return chip_of((place + hops) % chips, chips)

    def tokens_of(c, who):
        return pl.ds(pl.multiple_of(c * size + who * half, LANES), half)

    def piece(slot, c, s, way):
        if s == steps - 1:
            return held.at[slot, pl.ds(c * half + way * (half // 2), half // 2), :]
        return held.at[slot, pl.ds(c * half, half), :]

    def cols_of(who):
        return pl.ds(pl.multiple_of(who * depth, depth), depth)

    def own_part(c, way):
        return (
            h_ref.at[tokens_of(c, core), :],
            held.at[chip, pl.ds(c * half, half), cols_of(core)],
            side_send.at[way, c], side_recv.at[way, c], nexts[way],
        )

    def mate_part(c, way):
        part = held.at[chip, pl.ds(c * half, half), cols_of(1 - core)]
        return part, part, ring_send.at[way, 0, c], ring_recv.at[way, 0, c], nexts[way]

    def swap(c, who):
        return (
            h_ref.at[tokens_of(c, 1 - who), :],
            held.at[chip, pl.ds(c * half, half), cols_of(who)],
            own_send.at[c], own_recv.at[c], mate,
        )

    def begin(c):
        for way in range(2):
            start(*own_part(c, way))

    def begin_mate(c):
        remote(*swap(c, 1 - core)).wait_recv()
        for way in range(2):
            start(*mate_part(c, way))

    def arrive(c, s):
        for way in range(2):
            slot = source_of(way, s + 1)
            if s == 0:
                for who, send, recv in (
                    (core, side_send, side_recv.at[way, c]),
                    (1 - core, side_send, ring_recv.at[way, 0, c]),
                ):
                    here = held.at[slot, pl.ds(c * half, half), cols_of(who)]
                    remote(here, here, send.at[way, c], recv, nexts[way]).wait_recv()
            else:
                here = piece(slot, c, s, way)
                remote(
                    here, here, ring_send.at[way, s, c], ring_recv.at[way, s, c], nexts[way]
                ).wait_recv()
            if s + 1 < steps:
                on = piece(slot, c, s + 1, way)
                start(
                    on, on, ring_send.at[way, s + 1, c], ring_recv.at[way, s + 1, c], nexts[way]
                )

    wide = vocab
    per_core = vocab // wide

    def consume(c, loaders, first=False):
        rows = pl.ds(c * half, half)

        def body(n, carry):
            who = n // per_core
            cols = pl.ds(pl.multiple_of(n % per_core * wide, wide), wide)
            outs = pl.ds(pl.multiple_of(n * wide, wide), wide)
            value = 0.0 if first else logits[rows, outs]
            for load, deep in loaders:
                value += jnp.dot(
                    load(), w_ref[who, deep, cols], preferred_element_type=jnp.float32
                )
            logits[rows, outs] = value
            return carry

        lax.fori_loop(0, 2 * per_core, body, 0)
        side = 0.0 if first else left[c, core, :, 0:rank]
        for load, deep in loaders:
            side += lax.dot_general(
                load(), pin_ref[:, deep], ACROSS, preferred_element_type=jnp.float32
            )
        left[c, core, :, 0:rank] = side

    def deep_of(device):
        return pl.ds(pl.multiple_of(device * depth, depth), depth)

    def own_loaders(c):
        rows = pl.ds(c * half, half)
        return [
            (lambda: h_ref[tokens_of(c, core), :], deep_of(me)),
            (lambda: held[chip, rows, cols_of(1 - core)], deep_of(mate)),
        ]

    def step_loaders(c, s):
        rows = pl.ds(c * half, half)
        loaders = []
        for way in range(2 if s < steps - 1 else 1):
            slot = source_of(way, s + 1)
            deep = pl.ds(pl.multiple_of(slot * 2 * depth, 2 * depth), 2 * depth)
            loaders.append((lambda slot=slot: held[slot, rows, :], deep))
        return loaders

    lane = lax.broadcasted_iota(jnp.int32, (LANES, LANES), 1)
    inside = lane < rank
    base = lax.broadcasted_iota(jnp.int32, (LANES, 2 * vocab), 1) // LANES * LANES

    def spread_lanes(value):
        return jnp.concatenate([value] * (2 * vocab // LANES), axis=1)

    mates = [
        (pa_mine, pa_mine, mate_send.at[0], mate_recv.at[0], mate),
        (pb_mine, pb_mine, mate_send.at[1], mate_recv.at[1], mate),
        (w_hbm, w_ref.at[core], mate_send.at[2], mate_recv.at[2], mate),
    ]
    other_cols = pl.ds(pl.multiple_of((1 - core) * vocab, vocab), vocab)
    theirs = [
        pa_ref.at[0:rank, other_cols], pb_ref.at[rank : 2 * rank, other_cols],
        w_ref.at[1 - core],
    ]

    def from_mate(n):
        remote(theirs[n], theirs[n], mate_send.at[n], mate_recv.at[n], mate).wait_recv()

    def clear():
        pa_ref[rank : 2 * rank, :] = jnp.zeros((rank, 2 * vocab), jnp.bfloat16)
        pb_ref[0:rank, :] = jnp.zeros((rank, 2 * vocab), jnp.bfloat16)
        for c in range(chunks):
            left[c, core] = jnp.zeros((half, LANES), jnp.float32)
        grads[...] = jnp.zeros_like(grads)

    def prepare(c):
        for i in range(tiles):
            rows = pl.ds(c * half + i * LANES, LANES)
            spot = pl.ds(pl.multiple_of(c * size + core * half + i * LANES, LANES), LANES)
            wanted = jnp.broadcast_to(tgt_ref[:, spot].astype(jnp.float32), (LANES, LANES))
            wanted = jnp.transpose(wanted).astype(jnp.int32) - 2 * chip * vocab - lane
            shift[rows, :] = wanted
            onehot = jnp.where(spread_lanes(wanted) == base, 1.0, 0.0).astype(jnp.bfloat16)
            hot[rows, :] = lax.dot_general(
                onehot, pb_ref[...], ACROSS, preferred_element_type=jnp.float32
            )

    tiles = half // LANES

    def pack(values):
        packed = jnp.zeros((LANES, LANES), jnp.float32)
        for at, each in enumerate(values):
            packed = jnp.where(lane == at, each, packed)
        return packed

    def left_copy(c, who):
        return left.at[c, who], left.at[c, who], left_send.at[c], left_recv.at[c], mate

    def rs_copies(c, there):
        peer = 2 * there + core
        away = (there + chips - chip) % chips
        rows = pl.ds(pl.multiple_of(there * block, block), block)
        return [
            (msg.at[c, rows, :], got_msg.at[c, chip], msg_send.at[c, away], msg_recv.at[c, away],
             peer),
            (small.at[c, there], got_stat.at[c, chip], stat_send.at[c, away],
             stat_recv.at[c, away], peer),
        ]

    def soften(c):
        start(*left_copy(c, core))
        row = lax.broadcasted_iota(jnp.int32, (8, LANES), 0)
        spot = lax.broadcasted_iota(jnp.int32, (8, LANES), 1) // block
        keep = jnp.logical_and(row == spot, row < 3)
        per = LANES // block
        for i in range(tiles):
            rows = pl.ds(c * half + i * LANES, LANES)
            value = logits[rows, :]
            top = jnp.max(value, axis=1, keepdims=True)
            expo = jnp.exp(value - top)
            rest = jnp.where(spread_lanes(shift[rows, :]) == base, 0.0, expo)
            total = jnp.sum(expo, axis=1, keepdims=True)
            others = jnp.sum(rest, axis=1, keepdims=True)
            both = hot[rows, :] + lax.dot_general(
                rest.astype(jnp.bfloat16), pa_ref[...], ACROSS,
                preferred_element_type=jnp.float32,
            )
            msg[c, i * LANES : (i + 1) * LANES, :] = both.astype(jnp.bfloat16)
            line = jnp.transpose(pack([top, total, others]))[0:8, :]
            line = pltpu.roll(line, 0, 1, stride=block, stride_axis=0)
            for k in range(per):
                turn = pltpu.roll(line, (LANES - k * block) % LANES, 1)
                small[c, i * per + k] = jnp.sum(
                    jnp.where(keep, turn, 0.0), axis=0, keepdims=True
                )
        for k in range(1, chips):
            for copy in rs_copies(c, (chip + k) % chips):
                remote(*copy).start()
        got_msg[c, chip] = msg[c, pl.ds(pl.multiple_of(chip * block, block), block), :]
        got_stat[c, chip] = small[c, chip]

    fold = half // 2
    beside = lax.broadcasted_iota(jnp.int32, (fold, LANES), 1) < rank
    late = [(hot_late, got_hot), (msg_late, got_late), (line_late, got_line)]

    def late_copy(n, k):
        src, dst = late[n]
        there = (chip + k) % chips
        return src, dst.at[chip], late_send.at[n, k], late_recv.at[n, k], 2 * there + core

    def late_wait(n):
        for k in range(1, chips):
            there = (chip + chips - k) % chips
            spot = late[n][1].at[there]
            remote(
                spot, spot, late_send.at[n, k], late_recv.at[n, k], 2 * there + core
            ).wait_recv()

    def late_push(n):
        for k in range(1, chips):
            start(*late_copy(n, k))
        late[n][1][chip] = late[n][0][...]

    def push_hot():
        upper = hot[last * half : last * half + fold, :]
        lower = hot[last * half + fold : (last + 1) * half, :]
        hot_late[...] = jnp.where(beside, pltpu.roll(upper, rank, 1), lower).astype(jnp.bfloat16)
        late_push(0)

    def sum_hot():
        late_wait(0)
        value = jnp.zeros((fold, LANES), jnp.float32)
        for d in range(chips):
            value += got_hot[d].astype(jnp.float32)
        hot_sum[...] = value

    def soften_late():
        start(*left_copy(last, core))
        sums = []
        for i in range(tiles):
            rows = pl.ds(last * half + i * LANES, LANES)
            value = logits[rows, :]
            top = jnp.max(value, axis=1, keepdims=True)
            expo = jnp.exp(value - top)
            rest = jnp.where(spread_lanes(shift[rows, :]) == base, 0.0, expo)
            total = jnp.sum(expo, axis=1, keepdims=True)
            others = jnp.sum(rest, axis=1, keepdims=True)
            sums.append(lax.dot_general(
                rest.astype(jnp.bfloat16), pa_ref[...], ACROSS,
                preferred_element_type=jnp.float32,
            ))
            line_late[i] = jnp.transpose(pack([top, total, others]))[0:8, :]
        late_push(2)
        value = jnp.concatenate(sums, axis=0)
        msg_late[...] = jnp.where(
            beside, value[0:fold, :], pltpu.roll(value[fold:half, :], rank, 1)
        ).astype(jnp.bfloat16)
        late_push(1)

    def late_swap(who):
        return rights_late.at[who], rights_late.at[who], swap_send, swap_recv, mate

    def settle_late():
        late_wait(2)
        tables = []
        for i in range(tiles):
            lines = [got_line[d, i] for d in range(chips)]
            top = functools.reduce(jnp.maximum, [each[0:1, :] for each in lines])
            scale = [jnp.exp(each[0:1, :] - top) for each in lines]
            total = sum(scale[d] * lines[d][1:2, :] for d in range(chips))
            others = sum(scale[d] * lines[d][2:3, :] for d in range(chips))
            table = jnp.concatenate(
                [each / total for each in scale]
                + [
                    jnp.broadcast_to(others / total, (8, LANES)),
                    jnp.zeros((LANES - chips - 8, LANES), jnp.float32),
                ],
                axis=0,
            )
            tables.append(jnp.transpose(table))
        table = jnp.concatenate(tables, axis=0)

        def column(d):
            return jnp.where(beside, table[0:fold, d : d + 1], table[fold:half, d : d + 1])

        right = -column(chips) * hot_sum[...]
        factors = [column(d) for d in range(chips)]
        late_wait(1)
        for d in range(chips):
            right += factors[d] * got_late[d].astype(jnp.float32)
        rights_late[core] = right.astype(jnp.bfloat16)
        start(*late_swap(core))

    place_in = core * chips + chip

    def gather_copy(c, k):
        peer = (me + k) % devices
        spot = rights.at[c, place_in]
        return spot, spot, right_send.at[c, k], right_recv.at[c, k], peer

    def reduce(c):
        for k in range(1, chips):
            there = (chip + chips - k) % chips
            for dst, send, recv in (
                (got_msg.at[c, there], msg_send.at[c, k], msg_recv.at[c, k]),
                (got_stat.at[c, there], stat_send.at[c, k], stat_recv.at[c, k]),
            ):
                remote(dst, dst, send, recv, 2 * there + core).wait_recv()
        lines = jnp.concatenate([got_stat[c, d] for d in range(chips)], axis=0)
        top = jnp.max(lines, axis=0, keepdims=True)
        scale = jnp.exp(lines - top)
        total = jnp.sum(scale * pltpu.roll(lines, LANES - block, 1), axis=0, keepdims=True)
        others = jnp.sum(scale * pltpu.roll(lines, LANES - 2 * block, 1), axis=0, keepdims=True)
        table = jnp.concatenate(
            [
                scale / total,
                jnp.broadcast_to(others / total, (8, LANES)),
                jnp.zeros((LANES - chips - 8, LANES), jnp.float32),
            ],
            axis=0,
        )
        table = jnp.transpose(table)[0:block, :]
        summed = jnp.zeros((block, LANES), jnp.float32)
        plain = jnp.zeros((block, LANES), jnp.float32)
        for d in range(chips):
            value = got_msg[c, d].astype(jnp.float32)
            summed += value * table[:, d : d + 1]
            plain += value
        right = summed - table[:, chips : chips + 1] * pltpu.roll(plain, rank, 1)
        low, high = right[0 : block // 2, :], right[block // 2 : block, :]
        packed = jnp.where(inside[0 : block // 2, :], low, pltpu.roll(high, rank, 1))
        rights[c, place_in] = packed.astype(jnp.bfloat16)
        for k in range(1, devices):
            start(*gather_copy(c, k))

    def mark_docs(c):
        cols = pl.ds(c * size, size)
        remote(*left_copy(c, 1 - core)).wait_recv()
        turned[...] = jnp.transpose(left[c].reshape(size, LANES))
        member = seg_ref[:, cols] == lax.broadcasted_iota(jnp.int32, (docs, size), 0)

        def body(p, carry):
            rows = pl.ds(pl.multiple_of(p * docs, docs), docs)
            for side in range(2):
                line = turned[pl.ds(2 * p + side, 1), :]
                spread[c, rows, side * size : (side + 1) * size] = jnp.where(
                    member, line, 0.0
                ).astype(jnp.bfloat16)
            return carry

        lax.fori_loop(0, rank // 2, body, 0)

    def add_docs(c):
        if c == last:
            remote(*late_swap(1 - core)).wait_recv()
            packed, owning = rights_late[...].astype(jnp.float32), 1
        else:
            for k in range(1, devices):
                peer = (me + devices - k) % devices
                spot = rights.at[c, peer % 2 * chips + peer // 2]
                remote(spot, spot, right_send.at[c, k], right_recv.at[c, k], peer).wait_recv()
            packed, owning = rights[c].astype(jnp.float32), chips
        packed = packed.reshape(half, LANES)
        moved = pltpu.roll(packed, rank, 1)
        shape = (2 * owning, 1, fold // owning, LANES)
        both = jnp.concatenate([packed.reshape(shape), moved.reshape(shape)], axis=1)
        both = both.reshape(size, LANES)
        within = lax.broadcasted_iota(jnp.int32, (size, LANES), 1) < rank
        sides = jnp.concatenate(
            [jnp.where(within, both, 0.0), jnp.where(within, 0.0, pltpu.roll(both, rank, 1))],
            axis=0,
        ).astype(jnp.bfloat16)
        grads[...] += jnp.dot(spread[c], sides, preferred_element_type=jnp.float32)

    def query_rows(k):
        return qs.at[pl.ds(k * number, number), :]

    order = wavefront(chunks, steps)
    ahead = min(AHEAD, chunks)
    for c in range(ahead):
        begin(c)
    for c in range(chunks):
        start(*swap(c, core))
    pa_load.wait()
    pb_load.wait()
    for copy in mates:
        start(*copy)
    for k in range(1, groups):
        start(
            q_hbm, query_rows(groups - k), q_send.at[k], q_recv.at[k], None,
            (group + k) % groups,
        )
    for c in range(ahead):
        begin_mate(c)
    clear()
    tgt_load.wait()
    from_mate(0)
    from_mate(1)
    for c in range(chunks):
        prepare(c)

    def weights():
        w_load.wait()
        pin_load.wait()
        seg_load.wait()
        from_mate(2)

    tasks = [weights]
    ready = {c: own_loaders(c) for c in range(chunks)}

    def take(c, s):
        ready[c] += step_loaders(c, s)
        if s % 2 == 0 or s == steps - 1:
            tasks.append(functools.partial(consume, c, ready[c], s == 0))
            ready[c] = []
        if s == steps - 1:
            tasks.append(functools.partial(soften, c))
            if c == 0:
                tasks.append(push_hot)
            if c < last - 1:
                tasks.append(functools.partial(mark_docs, c))
            if c == 1 and c < last:
                tasks.append(sum_hot)

    ends = []
    for n, (c, s) in enumerate(order[ahead:]):
        if s == 0:
            begin(c)
            begin_mate(c)
            continue
        arrive(c, s - 1)
        take(c, s - 1)
        if s == steps - 1:
            ends.append((n + 2, c))
        while ends and ends[0][0] <= n and len(ends) > 1:
            c = ends.pop(0)[1]
            arrive(c, steps - 1)
            take(c, steps - 1)
        for _ in range(3):
            if tasks and n >= HOLD:
                tasks.pop(0)()
    while len(ends) > 1:
        c = ends.pop(0)[1]
        arrive(c, steps - 1)
        take(c, steps - 1)
        while tasks:
            tasks.pop(0)()
    while tasks:
        tasks.pop(0)()
    arrive(last, steps - 1)
    consume(last, step_loaders(last, steps - 1))
    soften_late()
    if last == 1:
        sum_hot()
    for c in range(last - 1):
        reduce(c)
    for c in range(max(last - 1, 0), chunks):
        mark_docs(c)
    if last > 0:
        reduce(last - 1)
    for c in range(last - 2):
        add_docs(c)
    settle_late()
    q_load.wait()
    for k in range(1, groups):
        remote(
            query_rows(k), query_rows(k), q_send.at[groups - k], q_recv.at[groups - k], None,
            (group + k) % groups,
        ).wait_recv()
    for c in range(max(last - 2, 0), chunks):
        add_docs(c)

    for p in range(rank // 2):
        flat[:, p * LANES : (p + 1) * LANES] = grads[p * docs : (p + 1) * docs, :].astype(
            jnp.bfloat16
        )
    mine = pl.ds(pl.multiple_of(group * docs, docs), docs)
    value = lax.dot_general(flat[...], qs[...], ACROSS, preferred_element_type=jnp.float32)
    for k in range(1, groups):
        scores[k] = value[:, k * number : (k + 1) * number]
        start(
            scores.at[k], out_ref.at[mine, :], group_send.at[k], group_recv.at[k], None,
            (group + k) % groups,
        )
    out_ref[mine, :] = value[:, 0:number]
    for k in range(1, groups):
        other = (group + groups - k) % groups
        theirs = out_ref.at[pl.ds(pl.multiple_of(other * docs, docs), docs), :]
        remote(
            theirs, theirs, group_send.at[k], group_recv.at[k], None, other
        ).wait_recv()
    for c in range(last):
        for k in range(1, chips):
            for copy in rs_copies(c, (chip + k) % chips):
                remote(*copy).wait_send()
    for copy in sent:
        copy.wait_send()


def attribution(devices, groups, hidden, weight, proj_in, proj_out, targets, segments, queries):
    tokens, depth = hidden.shape
    width, vocab = weight.shape
    rank = proj_in.shape[1]
    number = queries.shape[0]
    docs = DOC_V * devices
    chips, steps = devices // 2, devices // 4
    chunks = max(1, min(4, tokens // (2 * chips * BLOCK)))
    size = tokens // chunks
    half = size // 2
    block = half // chips
    hbm = pl.BlockSpec(memory_space=pl.ANY)
    dma = pltpu.SemaphoreType.DMA
    ring = dma((2, steps, chunks))
    once = dma((chunks,))
    sides = dma((2, chunks))
    peers = dma((chunks, chips))
    everyone = dma((chunks, devices))
    across = dma((groups,))
    f32, bf16 = jnp.float32, jnp.bfloat16
    return pl.pallas_call(
        functools.partial(kernel, devices, groups, chunks),
        out_shape=jax.ShapeDtypeStruct((groups * docs, number), f32),
        in_specs=[hbm] * 7,
        out_specs=pl.BlockSpec(memory_space=pltpu.VMEM),
        scratch_shapes=[
            pltpu.VMEM((tokens, depth), bf16),
            pltpu.VMEM((chips, tokens // 2, 2 * depth), bf16),
            pltpu.VMEM((2, width, vocab), bf16),
            pltpu.VMEM((rank, width), bf16),
            pltpu.VMEM((1, tokens), jnp.int32),
            pltpu.VMEM((1, tokens), jnp.int32),
            pltpu.VMEM((groups * number, rank * rank), bf16),
            pltpu.VMEM((tokens // 2, 2 * vocab), f32),
            pltpu.VMEM((chunks, 2, half, LANES), f32),
            pltpu.VMEM((tokens // 2, LANES), jnp.int32),
            pltpu.VMEM((LANES, 2 * vocab), bf16),
            pltpu.VMEM((LANES, 2 * vocab), bf16),
            pltpu.VMEM((tokens // 2, LANES), f32),
            pltpu.VMEM((LANES, size), f32),
            pltpu.VMEM((chunks, docs * rank // 2, 2 * size), bf16),
            pltpu.VMEM((chunks, half, LANES), bf16),
            pltpu.VMEM((chunks, chips, 1, LANES), f32),
            pltpu.VMEM((chunks, chips, block, LANES), bf16),
            pltpu.VMEM((chunks, chips, 1, LANES), f32),
            pltpu.VMEM((chunks, devices, block // 2, LANES), bf16),
            pltpu.VMEM((half // 2, LANES), bf16),
            pltpu.VMEM((chips, half // 2, LANES), bf16),
            pltpu.VMEM((half // 2, LANES), f32),
            pltpu.VMEM((half // 2, LANES), bf16),
            pltpu.VMEM((chips, half // 2, LANES), bf16),
            pltpu.VMEM((half // LANES, 8, LANES), f32),
            pltpu.VMEM((chips, half // LANES, 8, LANES), f32),
            pltpu.VMEM((2, half // 2, LANES), bf16),
            pltpu.VMEM((docs * rank // 2, LANES), f32),
            pltpu.VMEM((docs, rank * rank), bf16),
            pltpu.VMEM((groups, docs, number), f32),
            dma((8,)), ring, ring, sides, sides, once, once, dma((3,)), dma((3,)), once, once,
            peers, peers, peers, peers, everyone, everyone, dma((3, chips)), dma((3, chips)),
            dma(()), dma(()), across, across, across, across,
        ],
        compiler_params=pltpu.CompilerParams(
            collective_id=0, has_side_effects=True, vmem_limit_bytes=60 * 1024 * 1024
        ),
    )(
        hidden, weight, proj_in.T, proj_out.T, targets[None, :], segments, queries,
    )


def solution(mesh):
    devices, groups = mesh.shape["vocab"], mesh.shape["tok"]
    return jax.shard_map(
        functools.partial(attribution, devices, groups),
        mesh=mesh,
        in_specs=(
            P("tok", "vocab"),
            P(None, "vocab"),
            P(),
            P("vocab", None),
            P("tok"),
            P("tok", None),
            P(("vocab", "tok"), None),
        ),
        out_specs=P(None, ("vocab", "tok")),
        check_vma=False,
    )
```
